128 devices in a mesh: batch: 1, rows: 128 (over z, y, x, core).
Axes of the slice: x: 4, y: 4, z: 4, core: 2. Of those that a mesh axis runs over, the one named last changes fastest.
Arguments:
- a_mat: float32 [131072, 512], P(('batch', 'rows'))
- b_mat: float32 [131072, 512], P(('batch', 'rows'))
Outputs:
- output 1: float32 [131072, 512], P(('batch', 'rows'))
- output 2: float32 [512, 512], P('batch')
- output 3: float32 [131072, 512], P(('batch', 'rows'))
- output 4: float32 [512, 512], P('batch')
All inputs are finite; a program needn't handle non-finite values.
Results may differ from the reference program's by a relative error of at most 0.001.
Values sent between devices are 32-bit elements.
A program may use at most 1 GiB of HBM per device.

```python
import jax
import jax.numpy as jnp
from jax import lax

NUM_COLS = 512
ROWS_DEV = 1024
GROUP_SIZE = 128
TOTAL_ROWS = GROUP_SIZE * ROWS_DEV
COND_TARGET = 300.0
BOOST_SQ = 4.0


def draw_matrix(root_key):
    key_draw, key_rot = jax.random.split(root_key)
    gauss_draw = jax.random.normal(key_draw, (GROUP_SIZE, ROWS_DEV, NUM_COLS), jnp.float32)
    owner_ids = jnp.arange(NUM_COLS) % GROUP_SIZE
    col_boost = jnp.where(owner_ids[None, :] == jnp.arange(GROUP_SIZE)[:, None], (BOOST_SQ * GROUP_SIZE) ** 0.5, 1.0)
    weighted = (gauss_draw * col_boost[:, None, :]).reshape(TOTAL_ROWS, NUM_COLS)
    sing_vals = COND_TARGET ** (-jnp.arange(NUM_COLS, dtype=jnp.float32) / (NUM_COLS - 1))
    rotation = jnp.linalg.qr(jax.random.normal(key_rot, (NUM_COLS, NUM_COLS), jnp.float32))[0]
    mixing = sing_vals[:, None] * rotation.T
    return jnp.dot(weighted, mixing, precision=lax.Precision.HIGHEST, preferred_element_type=jnp.float32)


def setup_inputs(seed: int = 0, part: int = 0) -> dict:
    part_key = jax.random.fold_in(jax.random.key(seed), part)
    key_a, key_b = jax.random.split(part_key)
    return {"a_mat": draw_matrix(key_a), "b_mat": draw_matrix(key_b)}


def one_sweep(matrix):
    gram_sum = jnp.dot(matrix.T, matrix, precision=lax.Precision.HIGHEST, preferred_element_type=jnp.float32) / TOTAL_ROWS
    upper_fac = jnp.linalg.cholesky(gram_sum).T
    ortho_rows = lax.linalg.triangular_solve(upper_fac, matrix, left_side=False, lower=False)
    return ortho_rows, upper_fac


def cholesky_qr2(matrix):
    q_first, upper_first = one_sweep(matrix)
    q_final, upper_second = one_sweep(q_first)
    r_factor = jnp.dot(upper_second, upper_first, precision=lax.Precision.HIGHEST, preferred_element_type=jnp.float32)
    return q_final, r_factor


def reference(a_mat, b_mat):
    a_ortho, a_upper = cholesky_qr2(a_mat)
    b_ortho, b_upper = cholesky_qr2(b_mat)
    return (a_ortho, a_upper, b_ortho, b_upper)
```

```python
import functools

import jax
import jax.numpy as jnp
from jax import lax
from jax.experimental import pallas as pl
from jax.experimental.pallas import tpu as pltpu
from jax.sharding import PartitionSpec as P

FULL_PRECISION = lax.Precision.HIGHEST
F32 = jnp.float32
COLS = 512
ROWS = 1024
TILE = 128
BLOCKS = [(p, q) for p in range(4) for q in range(p, 4)]
PACKED = TILE * len(BLOCKS)
PART = PACKED // 4
PIECE = 24
PLANE = 16 * PIECE
VMEM = pl.BlockSpec(memory_space=pltpu.VMEM)
ANY = pl.BlockSpec(memory_space=pl.ANY)


def dot(a, b, ca, cb):
    return lax.dot_general(a, b, (((ca,), (cb,)), ((), ())), precision=FULL_PRECISION, preferred_element_type=F32)


def shape(*dims):
    return jax.ShapeDtypeStruct(dims, F32)


def row_of(x, k):
    return jnp.broadcast_to(x[k:k + 1, :], (8, TILE))


def col_of(x, k):
    return jnp.broadcast_to(x[:, k:k + 1], (8, TILE))


def factor_block(d_ref, w_ref):
    sub = lax.broadcasted_iota(jnp.int32, (8, TILE), 0)
    lane = lax.broadcasted_iota(jnp.int32, (8, TILE), 1)
    for kb in range(16):
        lo = 8 * kb
        rows = d_ref[lo:lo + 8, :]
        inv = w_ref[lo:lo + 8, :] + jnp.where(lane == sub + lo, 1.0, 0.0)
        cols = [col_of(rows, lo + j) for j in range(8)]
        scale, urow, wrow, low = [], [], [], {}
        for k in range(8):
            rs = lax.rsqrt(row_of(cols[k], k))
            lk = cols[k] * rs
            for j in range(k + 1, 8):
                low[j, k] = row_of(lk, j)
                cols[j] = cols[j] - lk * low[j, k]
            u, w = row_of(rows, k) * rs, row_of(inv, k) * rs
            lm = jnp.where(sub > k, lk, 0.0)
            rows = jnp.where(sub == k, u, rows - lm * u)
            inv = jnp.where(sub == k, w, inv - lm * w)
            scale.append(rs)
            urow.append(u)
            wrow.append(w)
        d_ref[lo:lo + 8, :] = jnp.where(lane >= sub + lo, rows, 0.0)
        w_ref[lo:lo + 8, :] = inv
        for m in range(kb + 1, 16):
            r = d_ref[8 * m:8 * m + 8, :]
            v = w_ref[8 * m:8 * m + 8, :]
            cs = [col_of(r, lo + j) for j in range(8)]
            for k in range(8):
                lk = cs[k] * scale[k]
                for j in range(k + 1, 8):
                    cs[j] = cs[j] - lk * low[j, k]
                r = r - lk * urow[k]
                v = v - lk * wrow[k]
            d_ref[8 * m:8 * m + 8, :] = r
            w_ref[8 * m:8 * m + 8, :] = v


def chol_kernel(g_ref, u_ref, m_ref, s_ref, d_ref, w_ref):
    s_ref[...] = jnp.zeros_like(s_ref)
    for i, (p, q) in enumerate(BLOCKS):
        s_ref[p, :, TILE * q:TILE * q + TILE] = g_ref[TILE * i:TILE * i + TILE, :]
    d_ref[...] = g_ref[0:TILE, :]

    def panel(p, carry):
        w_ref[...] = jnp.zeros_like(w_ref)
        factor_block(d_ref, w_ref)
        for pp in range(4):
            @pl.when(p == pp)
            def _():
                lo, hi = TILE * pp, TILE * pp + TILE
                w = w_ref[...]
                u_ref[lo:hi, :] = jnp.zeros((TILE, COLS), F32)
                m_ref[lo:hi, :] = jnp.zeros((TILE, COLS), F32)
                u_ref[lo:hi, lo:hi] = d_ref[...]
                m_ref[lo:hi, lo:hi] = w
                if pp > 0:
                    m_ref[lo:hi, 0:lo] = dot(w, s_ref[pp, :, 0:lo], 1, 0)
                if pp < 3:
                    right = dot(w, s_ref[pp, :, hi:], 1, 0)
                    u_ref[lo:hi, hi:] = right
                    for q in range(pp + 1, 4):
                        off = TILE * (q - pp - 1)
                        piece = right[:, off:off + TILE]
                        new = s_ref[q, :, TILE * q:] - dot(piece, right[:, off:], 0, 0)
                        s_ref[q, :, TILE * q:] = new
                        if q == pp + 1:
                            d_ref[...] = new[:, 0:TILE]
                        s_ref[q, :, 0:hi] = s_ref[q, :, 0:hi] - dot(piece, m_ref[lo:hi, 0:hi], 0, 0)
        return carry

    lax.fori_loop(0, 4, panel, 0)


def chol(gram):
    return pl.pallas_call(
        chol_kernel,
        name="chol",
        out_shape=[shape(COLS, COLS)] * 2,
        in_specs=[VMEM],
        out_specs=[VMEM, VMEM],
        scratch_shapes=[pltpu.VMEM((4, TILE, COLS), F32), pltpu.VMEM((TILE, TILE), F32), pltpu.VMEM((TILE, TILE), F32)],
    )(gram)


class Place:
    def __init__(self):
        self.me = lax.axis_index("rows")
        core = lax.rem(self.me, 2)
        x, y, z = (lax.rem(self.me // s, 4) for s in (2, 8, 32))
        self.core = core
        self.steps = (2 + 6 * core, 8 + 24 * core, 32 - 30 * core)
        self.spots = tuple(a + core * (b - a) for a, b in ((x, y), (y, z), (z, x)))
        self.partner = self.me + 1 - 2 * core

    def shifted(self, dim, j):
        spot = lax.rem(self.spots[dim] + j, 4)
        return spot, (spot - self.spots[dim]) * self.steps[dim]


PLANE_HOPS = [(j, k) for j in range(4) for k in range(4) if (j, k) != (0, 0)]


def remote(src, dst, send, recv, device):
    return pltpu.make_async_remote_copy(src_ref=src, dst_ref=dst, send_sem=send, recv_sem=recv, device_id={"rows": device}, device_id_type=pl.DeviceIdType.MESH)


def greet(place):
    barrier = pltpu.get_barrier_semaphore()
    peers = [place.partner]
    peers += [place.me + place.shifted(0, j)[1] for j in range(1, 4)]
    peers += [place.me + place.shifted(1, j)[1] + place.shifted(2, k)[1] for j, k in PLANE_HOPS]
    for peer in peers:
        pl.semaphore_signal(barrier, inc=1, device_id={"rows": peer}, device_id_type=pl.DeviceIdType.MESH)
    return lambda: pl.semaphore_wait(barrier, len(peers))


def sum_scratch():
    return [
        pltpu.VMEM((3, PART, TILE), F32),
        pltpu.VMEM((PLANE, TILE), F32),
        pltpu.VMEM((15, PIECE, TILE), F32),
        pltpu.VMEM((PLANE, TILE), F32),
        pltpu.VMEM((PACKED, TILE), F32),
        pltpu.SemaphoreType.DMA((2, 36)),
    ]


def ds(i, size):
    return pl.ds(pl.multiple_of(i * size, 8), size)


def all_sum(place, g_ref, got1, acc, got2, full, out, sems, inv_rows):
    copies = []

    def send(src, dst, device):
        copy = remote(src, dst, sems.at[0, len(copies)], sems.at[1, len(copies)], device)
        copy.start()
        copies.append(copy)
        return copy

    first = []
    for j in range(1, 4):
        spot, step = place.shifted(0, j)
        first.append(send(g_ref.at[ds(spot, PART)], got1.at[j - 1], place.me + step))
    acc[PART:, :] = jnp.zeros((PLANE - PART, TILE), F32)
    for copy in first:
        copy.wait_recv()
    acc[0:PART, :] = (g_ref[ds(place.spots[0], PART), :] + got1[0]) + (got1[1] + got1[2])
    second = []
    for i, (j, k) in enumerate(PLANE_HOPS):
        (spot1, step1), (spot2, step2) = place.shifted(1, j), place.shifted(2, k)
        second.append(send(acc.at[ds(spot1 * 4 + spot2, PIECE)], got2.at[i], place.me + step1 + step2))
    mine = place.spots[1] * 4 + place.spots[2]
    total = acc[ds(mine, PIECE), :]
    for i, copy in enumerate(second):
        copy.wait_recv()
        total = total + got2[i]
    full[ds(mine, PIECE), :] = total * inv_rows
    third = []
    for i, (j, k) in enumerate(PLANE_HOPS):
        step1, step2 = place.shifted(1, j)[1], place.shifted(2, k)[1]
        spot = full.at[ds(mine, PIECE)]
        third.append(send(spot, spot, place.me + step1 + step2))
    for copy in third:
        copy.wait_recv()
    last = []
    here = ds(place.spots[0], PART)
    for j in range(1, 4):
        last.append(send(full.at[0:PART], out.at[here], place.me + place.shifted(0, j)[1]))
    out[here, :] = full[0:PART, :]
    for copy in last:
        copy.wait_recv()
    for copy in copies:
        copy.wait_send()


def gram_into(x, dst):
    top = dot(x[:, 0:256], x[...], 0, 0)
    low = dot(x[:, 256:512], x[:, 256:512], 0, 0)
    for i, (p, q) in enumerate(BLOCKS):
        src, off = (top, 0) if p < 2 else (low, 256)
        dst[TILE * i:TILE * i + TILE, :] = src[TILE * p - off:TILE * p - off + TILE, TILE * q - off:TILE * q - off + TILE]


def first_kernel(inv_rows, a_ref, b_ref, out_ref, rows_ref, x, g, gx, local, swap, *scratch):
    place = Place()
    greeted = greet(place)
    for c, (other, own) in enumerate(((b_ref, a_ref), (a_ref, b_ref))):
        @pl.when(place.core == c)
        def _():
            pltpu.make_async_copy(other, x.at[0], local.at[0]).start()
            pltpu.make_async_copy(own, x.at[1], local.at[1]).start()
    pltpu.make_async_copy(a_ref, x.at[0], local.at[0]).wait()
    gram_into(x.at[0], g.at[0])
    greeted()
    give = remote(g.at[0], gx, swap.at[0], swap.at[1], place.partner)
    give.start()
    pltpu.make_async_copy(a_ref, x.at[1], local.at[1]).wait()
    gram_into(x.at[1], g.at[1])
    give.wait_recv()
    swap_rows = remote(x.at[0], rows_ref, swap.at[2], swap.at[3], place.partner)
    swap_rows.start()
    g[1] = g[1] + gx[...]
    *work, out, sems = scratch
    all_sum(place, g.at[1], *work, out, sems, inv_rows)
    out_ref[...] = out[...]
    give.wait_send()
    swap_rows.wait()


def first_sum(a, b, inv_rows):
    return pl.pallas_call(
        functools.partial(first_kernel, inv_rows),
        name="first_sum",
        out_shape=[shape(PACKED, TILE), shape(ROWS, COLS)],
        in_specs=[ANY, ANY],
        out_specs=[VMEM, ANY],
        scratch_shapes=[
            pltpu.VMEM((2, ROWS, COLS), F32),
            pltpu.VMEM((2, PACKED, TILE), F32),
            pltpu.VMEM((PACKED, TILE), F32),
            pltpu.SemaphoreType.DMA((2,)),
            pltpu.SemaphoreType.DMA((4,)),
            *sum_scratch(),
        ],
        compiler_params=pltpu.CompilerParams(collective_id=0, has_side_effects=True),
    )(a, b)


def solve_into(x, m, dst):
    dst[:, 0:256] = dot(x[:, 0:256], m[0:256, 0:256], 1, 1)
    dst[:, 256:512] = dot(x[...], m[256:512, :], 1, 1)


def second_kernel(inv_rows, a_ref, b_ref, rows_ref, m_ref, out_ref, own_ref, other_ref, x, q, g, local, swap, *scratch):
    place = Place()
    greeted = greet(place)
    for c, own in enumerate((a_ref, b_ref)):
        @pl.when(place.core == c)
        def _():
            pltpu.make_async_copy(own, x.at[1], local.at[1]).start()
    fetch = pltpu.make_async_copy(rows_ref, x.at[0], local.at[0])
    fetch.start()
    fetch.wait()
    solve_into(x.at[0], m_ref, q.at[0])
    greeted()
    swap_rows = remote(q.at[0], other_ref, swap.at[0], swap.at[1], place.partner)
    swap_rows.start()
    pltpu.make_async_copy(a_ref, x.at[1], local.at[1]).wait()
    solve_into(x.at[1], m_ref, q.at[1])
    keep = pltpu.make_async_copy(q.at[1], own_ref, local.at[2])
    keep.start()
    gram_into(q.at[0], g.at[0])
    gram_into(q.at[1], g.at[1])
    g[0] = g[0] + g[1]
    *work, out, sems = scratch
    all_sum(place, g.at[0], *work, out, sems, inv_rows)
    out_ref[...] = out[...]
    swap_rows.wait()
    keep.wait()


def second_sum(a, b, rows, m, inv_rows):
    return pl.pallas_call(
        functools.partial(second_kernel, inv_rows),
        name="second_sum",
        out_shape=[shape(PACKED, TILE), shape(ROWS, COLS), shape(ROWS, COLS)],
        in_specs=[ANY, ANY, ANY, VMEM],
        out_specs=[VMEM, ANY, ANY],
        scratch_shapes=[
            pltpu.VMEM((2, ROWS, COLS), F32),
            pltpu.VMEM((2, ROWS, COLS), F32),
            pltpu.VMEM((2, PACKED, TILE), F32),
            pltpu.SemaphoreType.DMA((3,)),
            pltpu.SemaphoreType.DMA((2,)),
            *sum_scratch(),
        ],
        compiler_params=pltpu.CompilerParams(collective_id=1, has_side_effects=True),
    )(a, b, rows, m)


def share_kernel(u1_ref, u2_ref, m_ref, ma_ref, mb_ref, ra_ref, rb_ref, r, got, sems):
    place = Place()
    barrier = pltpu.get_barrier_semaphore()
    pl.semaphore_signal(barrier, inc=1, device_id={"rows": place.partner}, device_id_type=pl.DeviceIdType.MESH)
    pl.semaphore_wait(barrier, 1)
    inv = remote(m_ref, got.at[0], sems.at[0], sems.at[1], place.partner)
    inv.start()
    r[...] = jnp.zeros_like(r)
    r[0:256, :] = dot(u2_ref[0:256, :], u1_ref[...], 1, 0)
    r[256:512, 256:512] = dot(u2_ref[256:512, 256:512], u1_ref[256:512, 256:512], 1, 0)
    tri = remote(r, got.at[1], sems.at[2], sems.at[3], place.partner)
    tri.start()
    inv.wait_recv()
    tri.wait_recv()
    for c, (m_own, m_other, r_own, r_other) in enumerate(((ma_ref, mb_ref, ra_ref, rb_ref), (mb_ref, ma_ref, rb_ref, ra_ref))):
        @pl.when(place.core == c)
        def _():
            m_own[...] = m_ref[...]
            r_own[...] = r[...]
            m_other[...] = got[0]
            r_other[...] = got[1]
    inv.wait_send()
    tri.wait_send()


def share(u1, u2, m):
    return pl.pallas_call(
        share_kernel,
        name="share",
        out_shape=[shape(COLS, COLS)] * 4,
        in_specs=[VMEM] * 3,
        out_specs=[VMEM] * 4,
        scratch_shapes=[pltpu.VMEM((COLS, COLS), F32), pltpu.VMEM((2, COLS, COLS), F32), pltpu.SemaphoreType.DMA((4,))],
        compiler_params=pltpu.CompilerParams(collective_id=2, has_side_effects=True),
    )(u1, u2, m)


def last_kernel(own_ref, other_ref, ma_ref, mb_ref, qa_ref, qb_ref):
    core = lax.rem(lax.axis_index("rows"), 2)
    for c, (qa, qb) in enumerate(((own_ref, other_ref), (other_ref, own_ref))):
        @pl.when(core == c)
        def _():
            solve_into(qa, ma_ref, qa_ref)
            solve_into(qb, mb_ref, qb_ref)


def last_solve(own, other, ma, mb):
    step = 256
    rows = pl.BlockSpec((step, COLS), lambda i: (i, 0))
    whole = pl.BlockSpec((COLS, COLS), lambda i: (0, 0))
    return pl.pallas_call(
        last_kernel,
        name="last_solve",
        grid=(ROWS // step,),
        out_shape=[shape(ROWS, COLS)] * 2,
        in_specs=[rows, rows, whole, whole],
        out_specs=[rows, rows],
    )(own, other, ma, mb)


def solution(mesh):
    row_spec = P(("batch", "rows"), None)
    tri_spec = P("batch", None)
    inv_rows = 1.0 / (ROWS * mesh.shape["rows"])

    def local_qr(a, b):
        gram1, rows = first_sum(a, b, inv_rows)
        u1, m1 = chol(gram1)
        gram2, own, other = second_sum(a, b, rows, m1, inv_rows)
        u2, m2 = chol(gram2)
        ma, mb, ra, rb = share(u1, u2, m2)
        qa, qb = last_solve(own, other, ma, mb)
        return qa, ra, qb, rb

    return jax.shard_map(local_qr, mesh=mesh, in_specs=(row_spec, row_spec), out_specs=(row_spec, tri_spec, row_spec, tri_spec), check_vma=False)
```

```python
import functools

import jax
import jax.numpy as jnp
from jax import lax
from jax.experimental import pallas as pl
from jax.experimental.pallas import tpu as pltpu
from jax.sharding import PartitionSpec as P

FULL_PRECISION = lax.Precision.HIGHEST
F32 = jnp.float32
COLS = 512
ROWS = 1024
TILE = 128
BLOCKS = [(p, q) for p in range(4) for q in range(p, 4)]
PACKED = TILE * len(BLOCKS)
FIRST = 112
PART = 4 * FIRST
PADDED = 3 * PART
PIECE = 8
PLANE = 16 * PIECE
CHUNK = 512
H = COLS // 2
MIB = 1 << 20
VMEM = pl.BlockSpec(memory_space=pltpu.VMEM)
HBM = pl.BlockSpec(memory_space=pltpu.HBM)


def dot(a, b, ca, cb):
    return lax.dot_general(a, b, (((ca,), (cb,)), ((), ())), precision=FULL_PRECISION, preferred_element_type=F32)


def shape(*dims):
    return jax.ShapeDtypeStruct(dims, F32)


def row_of(x, k):
    return jnp.broadcast_to(x[k:k + 1, :], (8, TILE))


def col_of(x, k):
    return jnp.broadcast_to(x[:, k:k + 1], (8, TILE))


def factor_block(d_ref, w_ref):
    sub = lax.broadcasted_iota(jnp.int32, (8, TILE), 0)
    lane = lax.broadcasted_iota(jnp.int32, (8, TILE), 1)
    for kb in range(16):
        lo = 8 * kb
        rows = d_ref[lo:lo + 8, :]
        inv = w_ref[lo:lo + 8, :] + jnp.where(lane == sub + lo, 1.0, 0.0)
        cols = [col_of(rows, lo + j) for j in range(8)]
        scale, urow, wrow, low = [], [], [], {}
        for k in range(8):
            rs = lax.rsqrt(row_of(cols[k], k))
            lk = cols[k] * rs
            for j in range(k + 1, 8):
                low[j, k] = row_of(lk, j)
                cols[j] = cols[j] - lk * low[j, k]
            u, w = row_of(rows, k) * rs, row_of(inv, k) * rs
            lm = jnp.where(sub > k, lk, 0.0)
            rows = jnp.where(sub == k, u, rows - lm * u)
            inv = jnp.where(sub == k, w, inv - lm * w)
            scale.append(rs)
            urow.append(u)
            wrow.append(w)
        d_ref[lo:lo + 8, :] = jnp.where(lane >= sub + lo, rows, 0.0)
        w_ref[lo:lo + 8, :] = inv
        for m in range(kb + 1, 16):
            r = d_ref[8 * m:8 * m + 8, :]
            v = w_ref[8 * m:8 * m + 8, :]
            cs = [col_of(r, lo + j) for j in range(8)]
            for k in range(8):
                lk = cs[k] * scale[k]
                for j in range(k + 1, 8):
                    cs[j] = cs[j] - lk * low[j, k]
                r = r - lk * urow[k]
                v = v - lk * wrow[k]
            d_ref[8 * m:8 * m + 8, :] = r
            w_ref[8 * m:8 * m + 8, :] = v


def factor_all(g_ref, u_ref, m_ref, s_ref, d_ref, w_ref):
    s_ref[...] = jnp.zeros_like(s_ref)
    for i, (p, q) in enumerate(BLOCKS):
        s_ref[TILE * p:TILE * p + TILE, TILE * q:TILE * q + TILE] = g_ref[TILE * i:TILE * i + TILE, :]
    d_ref[...] = g_ref[0:TILE, :]

    def panel(p, carry):
        w_ref[...] = jnp.zeros_like(w_ref)
        factor_block(d_ref, w_ref)
        for pp in range(4):
            @pl.when(p == pp)
            def _():
                lo, hi = TILE * pp, TILE * pp + TILE
                w = w_ref[...]
                u_ref[lo:hi, :] = jnp.zeros((TILE, COLS), F32)
                m_ref[lo:hi, :] = jnp.zeros((TILE, COLS), F32)
                u_ref[lo:hi, lo:hi] = d_ref[...]
                m_ref[lo:hi, lo:hi] = w
                if pp > 0:
                    m_ref[lo:hi, 0:lo] = dot(w, s_ref[lo:hi, 0:lo], 1, 0)
                if pp < 3:
                    right = dot(w, s_ref[lo:hi, hi:], 1, 0)
                    u_ref[lo:hi, hi:] = right
                    for q in range(pp + 1, 4):
                        off, band = TILE * (q - pp - 1), slice(TILE * q, TILE * q + TILE)
                        piece = right[:, off:off + TILE]
                        new = s_ref[band, TILE * q:] - dot(piece, right[:, off:], 0, 0)
                        s_ref[band, TILE * q:] = new
                        if q == pp + 1:
                            d_ref[...] = new[:, 0:TILE]
                        s_ref[band, 0:hi] = s_ref[band, 0:hi] - dot(piece, m_ref[lo:hi, 0:hi], 0, 0)
        return carry

    lax.fori_loop(0, 4, panel, 0)


def chol(gram):
    return pl.pallas_call(
        factor_all,
        name="chol",
        out_shape=[shape(COLS, COLS)] * 2,
        in_specs=[VMEM],
        out_specs=[VMEM, VMEM],
        scratch_shapes=[pltpu.VMEM((COLS, COLS), F32), pltpu.VMEM((TILE, TILE), F32), pltpu.VMEM((TILE, TILE), F32)],
        compiler_params=pltpu.CompilerParams(vmem_limit_bytes=MIB * 12),
        cost_estimate=pl.CostEstimate(flops=10**10, bytes_accessed=3 * MIB, transcendentals=COLS),
    )(gram)


def lower_half(x, edge):
    if not edge:
        return x
    row = lax.broadcasted_iota(jnp.int32, x.shape, 0)
    col = lax.broadcasted_iota(jnp.int32, x.shape, 1)
    return jnp.where(row > col, x, jnp.where(row == col, 0.5 * x, 0.0))


def near_identity_step(e_ref, n_ref):
    n00, n10, n11 = n_ref[0:H, 0:H], n_ref[H:, 0:H], n_ref[H:, H:]
    e00, e10, e11 = e_ref[0:H, 0:H], e_ref[H:, 0:H], e_ref[H:, H:]
    e01 = e_ref[0:H, H:]
    p00 = dot(n00, e00, 1, 0)
    p1 = dot(n_ref[H:, :], e_ref[...], 1, 0)
    p10, p11 = p1[:, 0:H], p1[:, H:]
    s00 = e00 + n00 + n00.T + p00 + dot(e00 + n00 + p00, n00, 1, 1)
    s10 = e10 + n10 + p10 + dot(e10 + n10 + p10, n00, 1, 1)
    s11 = e11 + n11 + n11.T + p11 + dot(e_ref[H:, :] + n_ref[H:, :] + p1, n_ref[H:, :], 1, 1)
    size = jnp.sum(s00 * s00) + 2 * jnp.sum(s10 * s10) + jnp.sum(s11 * s11)
    s00, s11 = lower_half(s00, True), lower_half(s11, True)
    n_ref[0:H, 0:H] = n00 - (s00 + dot(s00, n00, 1, 0))
    n_ref[H:, 0:H] = n10 - (s10 + dot(s10, n00, 1, 0) + dot(s11, n10, 1, 0))
    n_ref[H:, H:] = n11 - (s11 + dot(s11, n11, 1, 0))
    return size


def refine_kernel(g_ref, u1_ref, m_ref, r_ref, e_ref, n_ref, d_ref, w_ref):
    row = lax.broadcasted_iota(jnp.int32, (TILE, TILE), 0)
    col = lax.broadcasted_iota(jnp.int32, (TILE, TILE), 1)
    size = jnp.zeros((), F32)
    for i, (p, q) in enumerate(BLOCKS):
        x = g_ref[TILE * i:TILE * i + TILE, :]
        if p == q:
            x = x - jnp.where(row == col, 1.0, 0.0)
            n_ref[TILE * p:TILE * p + TILE, TILE * p:TILE * p + TILE] = -lower_half(x, True)
        else:
            t = x.T
            e_ref[TILE * q:TILE * q + TILE, TILE * p:TILE * p + TILE] = t
            n_ref[TILE * q:TILE * q + TILE, TILE * p:TILE * p + TILE] = -t
            n_ref[TILE * p:TILE * p + TILE, TILE * q:TILE * q + TILE] = jnp.zeros((TILE, TILE), F32)
        e_ref[TILE * p:TILE * p + TILE, TILE * q:TILE * q + TILE] = x
        size = size + (1 if p == q else 2) * jnp.sum(x * x)
    near = size < 0.1

    @pl.when(near)
    def _():
        lax.while_loop(lambda s: s > 1e-7, lambda s: near_identity_step(e_ref, n_ref), jnp.ones((), F32))
        n00, n1 = n_ref[0:H, 0:H], n_ref[H:, :]
        p0 = dot(n00, e_ref[0:H, :], 1, 0)
        p11 = dot(n1, e_ref[:, H:], 1, 0)
        f00 = e_ref[0:H, 0:H] + n00 + p0[:, 0:H]
        f01 = e_ref[0:H, H:] + p0[:, H:]
        f11 = e_ref[H:, H:] + n1[:, H:] + p11
        r2 = lax.broadcasted_iota(jnp.int32, (H, H), 0)
        c2 = lax.broadcasted_iota(jnp.int32, (H, H), 1)
        f00, f11 = jnp.where(r2 <= c2, f00, 0.0), jnp.where(r2 <= c2, f11, 0.0)
        r_ref[0:H, 0:H] = u1_ref[0:H, 0:H] + dot(f00, u1_ref[0:H, 0:H], 1, 0)
        r_ref[0:H, H:] = u1_ref[0:H, H:] + (dot(f00, u1_ref[0:H, H:], 1, 0) + dot(f01, u1_ref[H:, H:], 1, 0))
        r_ref[H:, 0:H] = jnp.zeros((H, H), F32)
        r_ref[H:, H:] = u1_ref[H:, H:] + dot(f11, u1_ref[H:, H:], 1, 0)
        for p in range(4):
            for q in range(4):
                x = n_ref[TILE * p:TILE * p + TILE, TILE * q:TILE * q + TILE]
                if p == q:
                    x = x + jnp.where(row == col, 1.0, 0.0)
                m_ref[TILE * p:TILE * p + TILE, TILE * q:TILE * q + TILE] = x

    @pl.when(jnp.logical_not(near))
    def _():
        factor_all(g_ref, e_ref, m_ref, n_ref, d_ref, w_ref)
        r_ref[0:H, :] = dot(e_ref[0:H, :], u1_ref[...], 1, 0)
        r_ref[H:, 0:H] = jnp.zeros((H, H), F32)
        r_ref[H:, H:] = dot(e_ref[H:, H:], u1_ref[H:, H:], 1, 0)

def refine(gram, u1):
    return pl.pallas_call(
        refine_kernel,
        name="refine",
        out_shape=[shape(COLS, COLS)] * 2,
        in_specs=[VMEM, VMEM],
        out_specs=[VMEM, VMEM],
        scratch_shapes=[pltpu.VMEM((COLS, COLS), F32)] * 2 + [pltpu.VMEM((TILE, TILE), F32)] * 2,
        compiler_params=pltpu.CompilerParams(vmem_limit_bytes=MIB * 16),
    )(gram, u1)


STEPS = (2, 8, 32)
HOPS = [(j, k) for j in range(4) for k in range(4) if (j, k) != (0, 0)]


class Place:
    def __init__(self):
        self.me = lax.axis_index("rows")
        self.core = lax.rem(self.me, 2)
        self.partner = self.me + 1 - 2 * self.core
        self.spots = tuple(lax.rem(self.me // step, 4) for step in STEPS)

    def shifted(self, dim, j):
        spot = lax.rem(self.spots[dim] + j, 4)
        return spot, (spot - self.spots[dim]) * STEPS[dim]


def remote(src, dst, send, recv, device):
    return pltpu.make_async_remote_copy(src_ref=src, dst_ref=dst, send_sem=send, recv_sem=recv, device_id={"rows": device}, device_id_type=pl.DeviceIdType.MESH)


def greet(place):
    barrier = pltpu.get_barrier_semaphore()
    peers = [place.partner]
    for dim in range(3):
        for j in range(1, 4):
            peers.append(place.me + place.shifted(dim, j)[1])
            peers += [place.me + place.shifted(dim, j)[1] + place.shifted((dim + 1) % 3, k)[1] for k in range(1, 4)]
    for peer in peers:
        pl.semaphore_signal(barrier, inc=1, device_id={"rows": peer}, device_id_type=pl.DeviceIdType.MESH)
    return lambda: pl.semaphore_wait(barrier, len(peers))


def sum_scratch():
    return [
        pltpu.VMEM((3, 3, FIRST, TILE), F32),
        pltpu.VMEM((3, PLANE, TILE), F32),
        pltpu.VMEM((3, 15, PIECE, TILE), F32),
        pltpu.VMEM((3, PLANE, TILE), F32),
        pltpu.VMEM((PADDED, TILE), F32),
        pltpu.SemaphoreType.DMA((2, 108)),
    ]


def span(start, size):
    return pl.ds(pl.multiple_of(start, 8), size)


def all_sum(place, g_ref, got1, acc, got2, full, out, sems, inv_rows, meanwhile):
    copies = []

    def send(src, dst, device):
        copy = remote(src, dst, sems.at[0, len(copies)], sems.at[1, len(copies)], device)
        copy.start()
        copies.append(copy)
        return copy

    def line(t):
        return [(j, *place.shifted(t, j)) for j in (2, 1, 3)]

    def plane(t):
        u, v = (t + 1) % 3, (t + 2) % 3
        for j, k in HOPS:
            (spot1, step1), (spot2, step2) = place.shifted(u, j), place.shifted(v, k)
            yield (spot1 * 4 + spot2) * PIECE, place.me + step1 + step2

    mine = [span(PART * t + place.spots[t] * FIRST, FIRST) for t in range(3)]
    piece = [span((place.spots[(t + 1) % 3] * 4 + place.spots[(t + 2) % 3]) * PIECE, PIECE) for t in range(3)]
    first, second, third, last = [], [], [], []
    for t in range(3):
        first.append([send(g_ref.at[span(PART * t + spot * FIRST, FIRST)], got1.at[t, j - 1], place.me + step) for j, spot, step in line(t)])
    meanwhile()
    for t in range(3):
        acc[t, FIRST:] = jnp.zeros((PLANE - FIRST, TILE), F32)
        for copy in first[t]:
            copy.wait_recv()
        acc[t, 0:FIRST] = (g_ref[mine[t], :] + got1[t, 0]) + (got1[t, 1] + got1[t, 2])
        second.append([send(acc.at[t, span(start, PIECE)], got2.at[t, i], device) for i, (start, device) in enumerate(plane(t))])
    for t in range(3):
        total = acc[t, piece[t]]
        for i, copy in enumerate(second[t]):
            copy.wait_recv()
            total = total + got2[t, i]
        full[t, piece[t]] = total * inv_rows
        spot = full.at[t, piece[t]]
        third.append([send(spot, spot, device) for _, device in plane(t)])
    for t in range(3):
        for copy in third[t]:
            copy.wait_recv()
        last.append([send(full.at[t, 0:FIRST], out.at[mine[t]], place.me + step) for _, _, step in line(t)])
        out[mine[t], :] = full[t, 0:FIRST]
    for t in range(3):
        for copy in last[t]:
            copy.wait_recv()
    for copy in copies:
        copy.wait_send()


def gram_add(x, top, low):
    top[...] = top[...] + dot(x[:, 0:H], x[...], 0, 0)
    low[...] = low[...] + dot(x[:, H:], x[:, H:], 0, 0)


def clear(*refs):
    for ref in refs:
        ref[...] = jnp.zeros_like(ref)


def pack(top, low, dst, extra=None):
    for i, (p, q) in enumerate(BLOCKS):
        src, off = (top, 0) if p < 2 else (low, H)
        x = src[TILE * p - off:TILE * p - off + TILE, TILE * q - off:TILE * q - off + TILE]
        here = slice(TILE * i, TILE * i + TILE)
        dst[here, :] = x if extra is None else x + extra[here, :]
    dst[PACKED:, :] = jnp.zeros((PADDED - PACKED, TILE), F32)


def first_kernel(inv_rows, a_ref, b_ref, out_ref, rows_ref, x, top, low, g, gx, local, swap, *scratch):
    place = Place()
    greeted = greet(place)
    chunks = ROWS // CHUNK

    def fetch(src, dst, half, i):
        return pltpu.make_async_copy(src.at[span(i * CHUNK, CHUNK)], dst.at[span(half * ROWS + i * CHUNK, CHUNK)], local.at[half, i])

    for c, (other, own) in enumerate(((b_ref, a_ref), (a_ref, b_ref))):
        @pl.when(place.core == c)
        def _():
            for i in range(chunks):
                fetch(other, x, 0, i).start()
            for i in range(chunks):
                fetch(own, rows_ref, 1, i).start()

    def add(half, src):
        def body(i, carry):
            fetch(a_ref, src, half, i).wait()
            gram_add(src.at[span(half * ROWS + i * CHUNK, CHUNK)], top, low)
            return carry
        clear(top, low)
        lax.fori_loop(0, chunks, body, 0)

    add(0, x)
    pack(top, low, g.at[0])
    greeted()
    give = remote(g.at[0], gx, swap.at[0], swap.at[1], place.partner)
    give.start()
    add(1, rows_ref)
    give.wait_recv()
    swap_rows = remote(x, rows_ref.at[0:ROWS], swap.at[2], swap.at[3], place.partner)
    pack(top, low, g.at[1], gx)
    *work, out, sems = scratch
    all_sum(place, g.at[1], *work, out, sems, inv_rows, swap_rows.start)
    out_ref[...] = out[0:PACKED, :]
    give.wait_send()
    swap_rows.wait()


def first_sum(a, b, inv_rows):
    return pl.pallas_call(
        functools.partial(first_kernel, inv_rows),
        name="first_sum",
        out_shape=[shape(PACKED, TILE), shape(2 * ROWS, COLS)],
        in_specs=[HBM, HBM],
        out_specs=[VMEM, VMEM],
        scratch_shapes=[
            pltpu.VMEM((ROWS, COLS), F32),
            pltpu.VMEM((H, COLS), F32),
            pltpu.VMEM((H, H), F32),
            pltpu.VMEM((2, PADDED, TILE), F32),
            pltpu.VMEM((PADDED, TILE), F32),
            pltpu.SemaphoreType.DMA((2, ROWS // CHUNK)),
            pltpu.SemaphoreType.DMA((4,)),
            *sum_scratch(),
        ],
        compiler_params=pltpu.CompilerParams(collective_id=0, vmem_limit_bytes=MIB * 52, has_side_effects=True),
    )(a, b)


def solve_into(x, m, dst):
    dst[:, 0:H] = dot(x[:, 0:H], m[0:H, 0:H], 1, 1)
    dst[:, H:] = dot(x[...], m[H:, :], 1, 1)


def second_kernel(inv_rows, rows_ref, m_ref, out_ref, q_ref, q, top, low, g, swap, *scratch):
    place = Place()
    greeted = greet(place)
    swap_rows = remote(q.at[0:ROWS], q_ref.at[0:ROWS], swap.at[0], swap.at[1], place.partner)
    clear(top, low)

    def body(i, carry):
        @pl.when(i == ROWS // CHUNK)
        def _():
            greeted()
            swap_rows.start()
        here = span(i * CHUNK, CHUNK)
        solve_into(rows_ref.at[here], m_ref, q.at[here])
        gram_add(q.at[here], top, low)
        return carry

    lax.fori_loop(0, 2 * ROWS // CHUNK, body, 0)
    pack(top, low, g)

    def keep():
        q_ref[ROWS:, :] = q[ROWS:, :]

    *work, out, sems = scratch
    all_sum(place, g, *work, out, sems, inv_rows, keep)
    out_ref[...] = out[0:PACKED, :]
    swap_rows.wait()


def second_sum(rows, m, inv_rows):
    return pl.pallas_call(
        functools.partial(second_kernel, inv_rows),
        name="second_sum",
        out_shape=[shape(PACKED, TILE), shape(2 * ROWS, COLS)],
        in_specs=[VMEM, VMEM],
        out_specs=[VMEM, VMEM],
        scratch_shapes=[
            pltpu.VMEM((2 * ROWS, COLS), F32),
            pltpu.VMEM((H, COLS), F32),
            pltpu.VMEM((H, H), F32),
            pltpu.VMEM((PADDED, TILE), F32),
            pltpu.SemaphoreType.DMA((2,)),
            *sum_scratch(),
        ],
        compiler_params=pltpu.CompilerParams(collective_id=1, vmem_limit_bytes=MIB * 24, has_side_effects=True),
    )(rows, m)


def share_kernel(m_ref, r_ref, m_out, r_out, sems):
    place = Place()
    barrier = pltpu.get_barrier_semaphore()
    pl.semaphore_signal(barrier, inc=1, device_id={"rows": place.partner}, device_id_type=pl.DeviceIdType.MESH)
    pl.semaphore_wait(barrier, 1)
    lo, hi, every = pl.ds(0, H), pl.ds(H, H), pl.ds(0, COLS)
    moves = [(m_ref, m_out, hi, every), (m_ref, m_out, lo, lo), (r_ref, r_out, lo, every), (r_ref, r_out, hi, hi)]
    copies = []
    for i, (src, dst, rows, cols) in enumerate(moves):
        copies.append(remote(src.at[rows, cols], dst.at[rows, cols], sems.at[0, i], sems.at[1, i], place.partner))
        copies[-1].start()
    m_out[lo, hi] = jnp.zeros((H, H), F32)
    r_out[hi, lo] = jnp.zeros((H, H), F32)
    for copy in copies:
        copy.wait()


def share(m, r):
    return pl.pallas_call(
        share_kernel,
        name="share",
        out_shape=[shape(COLS, COLS)] * 2,
        in_specs=[VMEM] * 2,
        out_specs=[VMEM] * 2,
        scratch_shapes=[pltpu.SemaphoreType.DMA((2, 4))],
        compiler_params=pltpu.CompilerParams(collective_id=2, vmem_limit_bytes=MIB * 8, has_side_effects=True),
    )(m, r)


def last_kernel(other_ref, own_ref, m_other, m_own, r_other, r_own, qa_ref, qb_ref, ra_ref, rb_ref):
    core = lax.rem(lax.axis_index("rows"), 2)
    for c, (q_own, q_other, ro, rp) in enumerate(((qa_ref, qb_ref, ra_ref, rb_ref), (qb_ref, qa_ref, rb_ref, ra_ref))):
        @pl.when(core == c)
        def _():
            solve_into(own_ref, m_own, q_own)
            solve_into(other_ref, m_other, q_other)
            ro[...] = r_own[...]
            rp[...] = r_other[...]


def last_solve(q, m_own, r_own, m_other, r_other):
    steps = 4
    rows = pl.BlockSpec((ROWS // steps, COLS), lambda i: (i, 0))
    more = pl.BlockSpec((ROWS // steps, COLS), lambda i: (i + steps, 0))
    tri = pl.BlockSpec((COLS // steps, COLS), lambda i: (i, 0))
    return pl.pallas_call(
        last_kernel,
        name="last_solve",
        grid=(steps,),
        out_shape=[shape(ROWS, COLS)] * 2 + [shape(COLS, COLS)] * 2,
        in_specs=[rows, more, VMEM, VMEM, tri, tri],
        out_specs=[rows, rows, tri, tri],
        compiler_params=pltpu.CompilerParams(vmem_limit_bytes=MIB * 16),
    )(q, q, m_other, m_own, r_other, r_own)


def solution(mesh):
    row_spec = P(("batch", "rows"), None)
    tri_spec = P("batch", None)
    inv_rows = 1.0 / (ROWS * mesh.shape["rows"])

    def local_qr(a, b):
        gram1, rows = first_sum(a, b, inv_rows)
        u1, m1 = chol(gram1)
        gram2, q = second_sum(rows, m1, inv_rows)
        m2, r = refine(gram2, u1)
        qa, qb, ra, rb = last_solve(q, m2, r, *share(m2, r))
        return qa, ra, qb, rb

    return jax.shard_map(local_qr, mesh=mesh, in_specs=(row_spec, row_spec), out_specs=(row_spec, tri_spec, row_spec, tri_spec), check_vma=False)
```

```python
import functools

import jax
import jax.numpy as jnp
from jax import lax
from jax.experimental import pallas as pl
from jax.experimental.pallas import tpu as pltpu
from jax.sharding import PartitionSpec as P

FULL_PRECISION = lax.Precision.HIGHEST
F32 = jnp.float32
COLS = 512
ROWS = 1024
TILE = 128
BLOCKS = [(p, q) for p in range(4) for q in range(p, 4)]
PACKED = TILE * len(BLOCKS)
FIRST = 112
PART = 4 * FIRST
PADDED = 3 * PART
PIECE = 32
PLANE = 4 * PIECE
CHUNK = 512
NEAR = 3
H = COLS // 2
MIB = 1 << 20
VMEM = pl.BlockSpec(memory_space=pltpu.VMEM)
HBM = pl.BlockSpec(memory_space=pltpu.HBM)


def dot(a, b, ca, cb):
    return lax.dot_general(a, b, (((ca,), (cb,)), ((), ())), precision=FULL_PRECISION, preferred_element_type=F32)


def shape(*dims):
    return jax.ShapeDtypeStruct(dims, F32)


def row_of(x, k):
    return jnp.broadcast_to(x[k:k + 1, :], (8, TILE))


def col_of(x, k):
    return jnp.broadcast_to(x[:, k:k + 1], (8, TILE))


def factor_block(d_ref, w_ref):
    sub = lax.broadcasted_iota(jnp.int32, (8, TILE), 0)
    lane = lax.broadcasted_iota(jnp.int32, (8, TILE), 1)
    tiles = TILE // 8
    at = [slice(8 * m, 8 * m + 8) for m in range(tiles)]
    cols = [col_of(d_ref[at[0], :], j) for j in range(8)]
    for kb in range(tiles):
        lo = 8 * kb
        held = d_ref[at[kb], :]
        rows = held
        inv = jnp.where(lane < lo, held, jnp.where(lane == sub + lo, 1.0, 0.0))
        done = lane < lo + 8
        here = (lane >= lo) & done
        ahead = kb + 1 < tiles
        if ahead:
            nxt = d_ref[at[kb + 1], :]
            side = [col_of(nxt, lo + j) for j in range(8)]
            coming = [col_of(nxt, lo + 8 + j) for j in range(8)]
            nxt = jnp.where(here, 0.0, nxt)
        low, both = {}, []
        scale = jnp.zeros((8, TILE), F32)
        for k in range(8):
            rs = lax.rsqrt(row_of(cols[k], k))
            ri = rs * rs
            for j in range(k + 1, 8):
                low[j, k] = row_of(cols[k], j) * ri
                cols[j] = cols[j] - cols[k] * low[j, k]
            if ahead:
                part = side[k] * ri
                for j in range(k + 1, 8):
                    side[j] = side[j] - side[k] * low[j, k]
                for j in range(8):
                    coming[j] = coming[j] - side[k] * row_of(part, j)
            u, w = row_of(rows, k) * ri, row_of(inv, k) * ri
            below = jnp.where(sub > k, cols[k], 0.0)
            rows = rows - below * u
            inv = inv - below * w
            scale = jnp.where(sub == k, rs, scale)
            both.append(jnp.where(done, w, u))
            if ahead:
                nxt = nxt - side[k] * both[k]
        d_ref[at[kb], :] = jnp.where(lane >= sub + lo, rows * scale, 0.0)
        w_ref[at[kb], :] = inv * scale
        if ahead:
            d_ref[at[kb + 1], :] = nxt
            cols = coming
        for m in range(kb + 2, tiles if kb >= tiles // 2 else tiles // 2 + NEAR):
            x = d_ref[at[m], :]
            side = [col_of(x, lo + j) for j in range(8)]
            x = jnp.where(here, 0.0, x)
            for k in range(8):
                for j in range(k + 1, 8):
                    side[j] = side[j] - side[k] * low[j, k]
                x = x - side[k] * both[k]
            d_ref[at[m], :] = x
        if kb == tiles // 2 - 1:
            half = TILE // 2
            upper = d_ref[0:half, :]
            wide = lax.broadcasted_iota(jnp.int32, (half, TILE), 1)
            band = dot(upper, jnp.where(wide < half, w_ref[0:half, :], upper), 0, 0)
            for m in range(tiles // 2 + NEAR, tiles):
                d_ref[at[m], :] = jnp.where(lane < half, 0.0, d_ref[at[m], :]) - band[at[m], :]


def factor_all(g_ref, u_ref, m_ref, s_ref, d_ref, w_ref):
    s_ref[...] = jnp.zeros_like(s_ref)
    for i, (p, q) in enumerate(BLOCKS):
        s_ref[TILE * p:TILE * p + TILE, TILE * q:TILE * q + TILE] = g_ref[TILE * i:TILE * i + TILE, :]
    d_ref[...] = g_ref[0:TILE, :]

    def panel(p, carry):
        factor_block(d_ref, w_ref)
        for pp in range(4):
            @pl.when(p == pp)
            def _():
                lo, hi = TILE * pp, TILE * pp + TILE
                w = w_ref[...]
                u_ref[lo:hi, :] = jnp.zeros((TILE, COLS), F32)
                m_ref[lo:hi, :] = jnp.zeros((TILE, COLS), F32)
                u_ref[lo:hi, lo:hi] = d_ref[...]
                m_ref[lo:hi, lo:hi] = w
                if pp > 0:
                    m_ref[lo:hi, 0:lo] = dot(w, s_ref[lo:hi, 0:lo], 1, 0)
                if pp < 3:
                    right = dot(w, s_ref[lo:hi, hi:], 1, 0)
                    u_ref[lo:hi, hi:] = right
                    for q in range(pp + 1, 4):
                        off, band = TILE * (q - pp - 1), slice(TILE * q, TILE * q + TILE)
                        piece = right[:, off:off + TILE]
                        new = s_ref[band, TILE * q:] - dot(piece, right[:, off:], 0, 0)
                        s_ref[band, TILE * q:] = new
                        if q == pp + 1:
                            d_ref[...] = new[:, 0:TILE]
                        s_ref[band, 0:hi] = s_ref[band, 0:hi] - dot(piece, m_ref[lo:hi, 0:hi], 0, 0)
        return carry

    lax.fori_loop(0, 4, panel, 0)


def chol(gram):
    return pl.pallas_call(
        factor_all,
        name="chol",
        out_shape=[shape(COLS, COLS)] * 2,
        in_specs=[VMEM],
        out_specs=[VMEM, VMEM],
        scratch_shapes=[pltpu.VMEM((COLS, COLS), F32), pltpu.VMEM((TILE, TILE), F32), pltpu.VMEM((TILE, TILE), F32)],
        compiler_params=pltpu.CompilerParams(vmem_limit_bytes=MIB * 12),
        cost_estimate=pl.CostEstimate(flops=10**10, bytes_accessed=3 * MIB, transcendentals=COLS),
    )(gram)


def lower_half(x, edge):
    if not edge:
        return x
    row = lax.broadcasted_iota(jnp.int32, x.shape, 0)
    col = lax.broadcasted_iota(jnp.int32, x.shape, 1)
    return jnp.where(row > col, x, jnp.where(row == col, 0.5 * x, 0.0))


def near_identity_step(e_ref, n_ref):
    n00, n10, n11 = n_ref[0:H, 0:H], n_ref[H:, 0:H], n_ref[H:, H:]
    e00, e10, e11 = e_ref[0:H, 0:H], e_ref[H:, 0:H], e_ref[H:, H:]
    e01 = e_ref[0:H, H:]
    p00 = dot(n00, e00, 1, 0)
    p1 = dot(n_ref[H:, :], e_ref[...], 1, 0)
    p10, p11 = p1[:, 0:H], p1[:, H:]
    s00 = e00 + n00 + n00.T + p00 + dot(e00 + n00 + p00, n00, 1, 1)
    s10 = e10 + n10 + p10 + dot(e10 + n10 + p10, n00, 1, 1)
    s11 = e11 + n11 + n11.T + p11 + dot(e_ref[H:, :] + n_ref[H:, :] + p1, n_ref[H:, :], 1, 1)
    size = jnp.sum(s00 * s00) + 2 * jnp.sum(s10 * s10) + jnp.sum(s11 * s11)
    s00, s11 = lower_half(s00, True), lower_half(s11, True)
    n_ref[0:H, 0:H] = n00 - (s00 + dot(s00, n00, 1, 0))
    n_ref[H:, 0:H] = n10 - (s10 + dot(s10, n00, 1, 0) + dot(s11, n10, 1, 0))
    n_ref[H:, H:] = n11 - (s11 + dot(s11, n11, 1, 0))
    return size


def refine_kernel(g_ref, u1_ref, m_ref, r_ref, e_ref, n_ref, d_ref, w_ref):
    row = lax.broadcasted_iota(jnp.int32, (TILE, TILE), 0)
    col = lax.broadcasted_iota(jnp.int32, (TILE, TILE), 1)
    size = jnp.zeros((), F32)
    for i, (p, q) in enumerate(BLOCKS):
        x = g_ref[TILE * i:TILE * i + TILE, :]
        if p == q:
            x = x - jnp.where(row == col, 1.0, 0.0)
            n_ref[TILE * p:TILE * p + TILE, TILE * p:TILE * p + TILE] = -lower_half(x, True)
        else:
            t = x.T
            e_ref[TILE * q:TILE * q + TILE, TILE * p:TILE * p + TILE] = t
            n_ref[TILE * q:TILE * q + TILE, TILE * p:TILE * p + TILE] = -t
            n_ref[TILE * p:TILE * p + TILE, TILE * q:TILE * q + TILE] = jnp.zeros((TILE, TILE), F32)
        e_ref[TILE * p:TILE * p + TILE, TILE * q:TILE * q + TILE] = x
        size = size + (1 if p == q else 2) * jnp.sum(x * x)
    near = size < 0.1

    @pl.when(near)
    def _():
        lax.while_loop(lambda s: s > 1e-7, lambda s: near_identity_step(e_ref, n_ref), jnp.ones((), F32))
        n00, n1 = n_ref[0:H, 0:H], n_ref[H:, :]
        p0 = dot(n00, e_ref[0:H, :], 1, 0)
        p11 = dot(n1, e_ref[:, H:], 1, 0)
        f00 = e_ref[0:H, 0:H] + n00 + p0[:, 0:H]
        f01 = e_ref[0:H, H:] + p0[:, H:]
        f11 = e_ref[H:, H:] + n1[:, H:] + p11
        r2 = lax.broadcasted_iota(jnp.int32, (H, H), 0)
        c2 = lax.broadcasted_iota(jnp.int32, (H, H), 1)
        f00, f11 = jnp.where(r2 <= c2, f00, 0.0), jnp.where(r2 <= c2, f11, 0.0)
        r_ref[0:H, 0:H] = u1_ref[0:H, 0:H] + dot(f00, u1_ref[0:H, 0:H], 1, 0)
        r_ref[0:H, H:] = u1_ref[0:H, H:] + (dot(f00, u1_ref[0:H, H:], 1, 0) + dot(f01, u1_ref[H:, H:], 1, 0))
        r_ref[H:, 0:H] = jnp.zeros((H, H), F32)
        r_ref[H:, H:] = u1_ref[H:, H:] + dot(f11, u1_ref[H:, H:], 1, 0)
        for p in range(4):
            for q in range(4):
                x = n_ref[TILE * p:TILE * p + TILE, TILE * q:TILE * q + TILE]
                if p == q:
                    x = x + jnp.where(row == col, 1.0, 0.0)
                m_ref[TILE * p:TILE * p + TILE, TILE * q:TILE * q + TILE] = x

    @pl.when(jnp.logical_not(near))
    def _():
        factor_all(g_ref, e_ref, m_ref, n_ref, d_ref, w_ref)
        r_ref[0:H, :] = dot(e_ref[0:H, :], u1_ref[...], 1, 0)
        r_ref[H:, 0:H] = jnp.zeros((H, H), F32)
        r_ref[H:, H:] = dot(e_ref[H:, H:], u1_ref[H:, H:], 1, 0)

def refine(gram, u1):
    return pl.pallas_call(
        refine_kernel,
        name="refine",
        out_shape=[shape(COLS, COLS)] * 2,
        in_specs=[VMEM, VMEM],
        out_specs=[VMEM, VMEM],
        scratch_shapes=[pltpu.VMEM((COLS, COLS), F32)] * 2 + [pltpu.VMEM((TILE, TILE), F32)] * 2,
        compiler_params=pltpu.CompilerParams(vmem_limit_bytes=MIB * 16),
    )(gram, u1)


STEPS = (2, 8, 32)


class Place:
    def __init__(self):
        self.me = lax.axis_index("rows")
        self.core = lax.rem(self.me, 2)
        self.partner = self.me + 1 - 2 * self.core
        self.spots = tuple(lax.rem(self.me // step, 4) for step in STEPS)

    def shifted(self, dim, j):
        spot = lax.rem(self.spots[dim] + j, 4)
        return spot, (spot - self.spots[dim]) * STEPS[dim]


def remote(src, dst, send, recv, device):
    return pltpu.make_async_remote_copy(src_ref=src, dst_ref=dst, send_sem=send, recv_sem=recv, device_id={"rows": device}, device_id_type=pl.DeviceIdType.MESH)


def greet(place):
    barrier = pltpu.get_barrier_semaphore()
    peers = [place.partner] + [place.me + place.shifted(dim, j)[1] for dim in range(3) for j in range(1, 4)]
    for peer in peers:
        pl.semaphore_signal(barrier, inc=1, device_id={"rows": peer}, device_id_type=pl.DeviceIdType.MESH)
    return lambda: pl.semaphore_wait(barrier, len(peers))


def sum_scratch():
    return [
        pltpu.VMEM((3, 3, FIRST, TILE), F32),
        pltpu.VMEM((3, PLANE, TILE), F32),
        pltpu.VMEM((3, 3, PIECE, TILE), F32),
        pltpu.VMEM((3, 4, PIECE, TILE), F32),
        pltpu.VMEM((3, PLANE, TILE), F32),
        pltpu.VMEM((PADDED, TILE), F32),
        pltpu.SemaphoreType.DMA((2, 45)),
    ]


def span(start, size):
    return pl.ds(pl.multiple_of(start, 8), size)


def all_sum(place, g_ref, got1, acc, got2, terms, full, out, sems, inv_rows, meanwhile):
    copies = []

    def send(src, dst, device):
        copy = remote(src, dst, sems.at[0, len(copies)], sems.at[1, len(copies)], device)
        copy.start()
        copies.append(copy)
        return copy

    def line(dim):
        return [(j, *place.shifted(dim, j)) for j in (2, 1, 3)]

    me, spots = place.me, place.spots
    mine = [span(PART * t + spots[t] * FIRST, FIRST) for t in range(3)]
    piece = [span(spots[(t + 1) % 3] * PIECE, PIECE) for t in range(3)]
    hops = [[] for _ in range(5)]
    for t in range(3):
        hops[0].append([send(g_ref.at[span(PART * t + spot * FIRST, FIRST)], got1.at[t, j - 1], me + step) for j, spot, step in line(t)])
    meanwhile()
    for t in range(3):
        acc[t, FIRST:] = jnp.zeros((PLANE - FIRST, TILE), F32)
        for copy in hops[0][t]:
            copy.wait_recv()
        acc[t, 0:FIRST] = (g_ref[mine[t], :] + got1[t, 0]) + (got1[t, 1] + got1[t, 2])
        hops[1].append([send(acc.at[t, span(spot * PIECE, PIECE)], got2.at[t, j - 1], me + step) for j, spot, step in line((t + 1) % 3)])
    for t in range(3):
        third = (t + 2) % 3
        for copy in hops[1][t]:
            copy.wait_recv()
        terms[t, spots[third]] = (acc[t, piece[t]] + got2[t, 0]) + (got2[t, 1] + got2[t, 2])
        term = terms.at[t, spots[third]]
        hops[2].append([send(term, term, me + step) for _, _, step in line(third)])
    for t in range(3):
        for copy in hops[2][t]:
            copy.wait_recv()
        full[t, piece[t]] = ((terms[t, 0] + terms[t, 1]) + (terms[t, 2] + terms[t, 3])) * inv_rows
        here = full.at[t, piece[t]]
        hops[3].append([send(here, here, me + step) for _, _, step in line((t + 1) % 3)])
    for t in range(3):
        for copy in hops[3][t]:
            copy.wait_recv()
        hops[4].append([send(full.at[t, 0:FIRST], out.at[mine[t]], me + step) for _, _, step in line(t)])
        out[mine[t], :] = full[t, 0:FIRST]
    for group in hops[4]:
        for copy in group:
            copy.wait_recv()
    for copy in copies:
        copy.wait_send()


def gram_add(x, top, low):
    top[...] = top[...] + dot(x[:, 0:H], x[...], 0, 0)
    low[...] = low[...] + dot(x[:, H:], x[:, H:], 0, 0)


def clear(*refs):
    for ref in refs:
        ref[...] = jnp.zeros_like(ref)


def pack(top, low, dst, extra=None):
    for i, (p, q) in enumerate(BLOCKS):
        src, off = (top, 0) if p < 2 else (low, H)
        x = src[TILE * p - off:TILE * p - off + TILE, TILE * q - off:TILE * q - off + TILE]
        here = slice(TILE * i, TILE * i + TILE)
        dst[here, :] = x if extra is None else x + extra[here, :]
    dst[PACKED:, :] = jnp.zeros((PADDED - PACKED, TILE), F32)


def first_kernel(inv_rows, a_ref, b_ref, out_ref, rows_ref, x, top, low, g, gx, local, swap, *scratch):
    place = Place()
    greeted = greet(place)
    chunks = ROWS // CHUNK

    def fetch(src, dst, half, i):
        return pltpu.make_async_copy(src.at[span(i * CHUNK, CHUNK)], dst.at[span(half * ROWS + i * CHUNK, CHUNK)], local.at[half, i])

    for c, (other, own) in enumerate(((b_ref, a_ref), (a_ref, b_ref))):
        @pl.when(place.core == c)
        def _():
            for i in range(chunks):
                fetch(other, x, 0, i).start()
            for i in range(chunks):
                fetch(own, rows_ref, 1, i).start()

    def add(half, src):
        def body(i, carry):
            fetch(a_ref, src, half, i).wait()
            gram_add(src.at[span(half * ROWS + i * CHUNK, CHUNK)], top, low)
            return carry
        clear(top, low)
        lax.fori_loop(0, chunks, body, 0)

    add(0, x)
    pack(top, low, g.at[0])
    greeted()
    give = remote(g.at[0], gx, swap.at[0], swap.at[1], place.partner)
    give.start()
    add(1, rows_ref)
    give.wait_recv()
    swap_rows = remote(x, rows_ref.at[0:ROWS], swap.at[2], swap.at[3], place.partner)
    pack(top, low, g.at[1], gx)
    *work, out, sems = scratch
    all_sum(place, g.at[1], *work, out, sems, inv_rows, swap_rows.start)
    out_ref[...] = out[0:PACKED, :]
    give.wait_send()
    swap_rows.wait()


def first_sum(a, b, inv_rows):
    return pl.pallas_call(
        functools.partial(first_kernel, inv_rows),
        name="first_sum",
        out_shape=[shape(PACKED, TILE), shape(2 * ROWS, COLS)],
        in_specs=[HBM, HBM],
        out_specs=[VMEM, VMEM],
        scratch_shapes=[
            pltpu.VMEM((ROWS, COLS), F32),
            pltpu.VMEM((H, COLS), F32),
            pltpu.VMEM((H, H), F32),
            pltpu.VMEM((2, PADDED, TILE), F32),
            pltpu.VMEM((PADDED, TILE), F32),
            pltpu.SemaphoreType.DMA((2, ROWS // CHUNK)),
            pltpu.SemaphoreType.DMA((4,)),
            *sum_scratch(),
        ],
        compiler_params=pltpu.CompilerParams(collective_id=0, vmem_limit_bytes=MIB * 52, has_side_effects=True),
    )(a, b)


def solve_into(x, m, dst):
    dst[:, 0:H] = dot(x[:, 0:H], m[0:H, 0:H], 1, 1)
    dst[:, H:] = dot(x[...], m[H:, :], 1, 1)


def second_kernel(inv_rows, rows_ref, m_ref, out_ref, q_ref, q, top, low, g, swap, *scratch):
    place = Place()
    greeted = greet(place)
    swap_rows = remote(q.at[0:ROWS], q_ref.at[0:ROWS], swap.at[0], swap.at[1], place.partner)
    clear(top, low)

    def body(i, carry):
        @pl.when(i == ROWS // CHUNK)
        def _():
            greeted()
            swap_rows.start()
        here = span(i * CHUNK, CHUNK)
        solve_into(rows_ref.at[here], m_ref, q.at[here])
        gram_add(q.at[here], top, low)
        return carry

    lax.fori_loop(0, 2 * ROWS // CHUNK, body, 0)
    pack(top, low, g)

    def keep():
        q_ref[ROWS:, :] = q[ROWS:, :]

    *work, out, sems = scratch
    all_sum(place, g, *work, out, sems, inv_rows, keep)
    out_ref[...] = out[0:PACKED, :]
    swap_rows.wait()


def second_sum(rows, m, inv_rows):
    return pl.pallas_call(
        functools.partial(second_kernel, inv_rows),
        name="second_sum",
        out_shape=[shape(PACKED, TILE), shape(2 * ROWS, COLS)],
        in_specs=[VMEM, VMEM],
        out_specs=[VMEM, VMEM],
        scratch_shapes=[
            pltpu.VMEM((2 * ROWS, COLS), F32),
            pltpu.VMEM((H, COLS), F32),
            pltpu.VMEM((H, H), F32),
            pltpu.VMEM((PADDED, TILE), F32),
            pltpu.SemaphoreType.DMA((2,)),
            *sum_scratch(),
        ],
        compiler_params=pltpu.CompilerParams(collective_id=1, vmem_limit_bytes=MIB * 24, has_side_effects=True),
    )(rows, m)


def share_kernel(m_ref, r_ref, m_out, r_out, sems):
    place = Place()
    barrier = pltpu.get_barrier_semaphore()
    pl.semaphore_signal(barrier, inc=1, device_id={"rows": place.partner}, device_id_type=pl.DeviceIdType.MESH)
    pl.semaphore_wait(barrier, 1)
    lo, hi, every = pl.ds(0, H), pl.ds(H, H), pl.ds(0, COLS)
    moves = [(m_ref, m_out, hi, every), (m_ref, m_out, lo, lo), (r_ref, r_out, lo, every), (r_ref, r_out, hi, hi)]
    copies = []
    for i, (src, dst, rows, cols) in enumerate(moves):
        copies.append(remote(src.at[rows, cols], dst.at[rows, cols], sems.at[0, i], sems.at[1, i], place.partner))
        copies[-1].start()
    m_out[lo, hi] = jnp.zeros((H, H), F32)
    r_out[hi, lo] = jnp.zeros((H, H), F32)
    for copy in copies:
        copy.wait()


def share(m, r):
    return pl.pallas_call(
        share_kernel,
        name="share",
        out_shape=[shape(COLS, COLS)] * 2,
        in_specs=[VMEM] * 2,
        out_specs=[VMEM] * 2,
        scratch_shapes=[pltpu.SemaphoreType.DMA((2, 4))],
        compiler_params=pltpu.CompilerParams(collective_id=2, vmem_limit_bytes=MIB * 8, has_side_effects=True),
    )(m, r)


def last_kernel(other_ref, own_ref, m_other, m_own, r_other, r_own, qa_ref, qb_ref, ra_ref, rb_ref):
    core = lax.rem(lax.axis_index("rows"), 2)
    for c, (q_own, q_other, ro, rp) in enumerate(((qa_ref, qb_ref, ra_ref, rb_ref), (qb_ref, qa_ref, rb_ref, ra_ref))):
        @pl.when(core == c)
        def _():
            solve_into(own_ref, m_own, q_own)
            solve_into(other_ref, m_other, q_other)
            ro[...] = r_own[...]
            rp[...] = r_other[...]


def last_solve(q, m_own, r_own, m_other, r_other):
    steps = 4
    rows = pl.BlockSpec((ROWS // steps, COLS), lambda i: (i, 0))
    more = pl.BlockSpec((ROWS // steps, COLS), lambda i: (i + steps, 0))
    tri = pl.BlockSpec((COLS // steps, COLS), lambda i: (i, 0))
    return pl.pallas_call(
        last_kernel,
        name="last_solve",
        grid=(steps,),
        out_shape=[shape(ROWS, COLS)] * 2 + [shape(COLS, COLS)] * 2,
        in_specs=[rows, more, VMEM, VMEM, tri, tri],
        out_specs=[rows, rows, tri, tri],
        compiler_params=pltpu.CompilerParams(vmem_limit_bytes=MIB * 16),
    )(q, q, m_other, m_own, r_other, r_own)


def solution(mesh):
    row_spec = P(("batch", "rows"), None)
    tri_spec = P("batch", None)
    inv_rows = 1.0 / (ROWS * mesh.shape["rows"])

    def local_qr(a, b):
        gram1, rows = first_sum(a, b, inv_rows)
        u1, m1 = chol(gram1)
        gram2, q = second_sum(rows, m1, inv_rows)
        m2, r = refine(gram2, u1)
        qa, qb, ra, rb = last_solve(q, m2, r, *share(m2, r))
        return qa, ra, qb, rb

    return jax.shard_map(local_qr, mesh=mesh, in_specs=(row_spec, row_spec), out_specs=(row_spec, tri_spec, row_spec, tri_spec), check_vma=False)
```
